32 devices in a mesh: dp: 4 (over x, core), tensor: 8 (over z, y).
Axes of the slice: x: 2, y: 2, z: 4, core: 2. Of those that a mesh axis runs over, the one named last changes fastest.
Arguments:
- out_grad: bfloat16 [2, 320, 4096], P(None, 'dp', 'tensor'), may hold values from -0.3125 to 0.3125
- layer_input: bfloat16 [2, 320, 4096], P(None, 'dp', 'tensor'), may hold values from -8 to 8
- w_down: bfloat16 [16384, 4096], P('tensor'), may hold values from -0.046875 to 0.046875
- silu_gate: bfloat16 [2, 320, 16384], P(None, 'dp', 'tensor'), may hold values from -6 to 6
- up_proj: bfloat16 [2, 320, 16384], P(None, 'dp', 'tensor'), may hold values from -6 to 6
- slope_codes: int32 [2, 32, 16384], P(None, 'dp', 'tensor'), may hold values from 0 to 1073741823
Outputs:
- grad_down: bfloat16 [16384, 4096], P('tensor', 'dp')
- grad_gate: bfloat16 [4096, 16384], P('dp', 'tensor')
- grad_up: bfloat16 [4096, 16384], P('dp', 'tensor')
The draws below stay inside these ranges and needn't reach their ends.
Inputs may be any that keep to these rules, and one draw needn't show every extreme that they name: `slope_codes`: every word holds ten independent 3-bit codes; all eight codes occur.
All inputs are finite; a program needn't handle non-finite values.
Results may differ from the reference program's by a relative error of at most 0.018.
Values may be sent and summed in bfloat16 or wider, within the bound.
No kernel may reach another device: no remote copies, remote signals or barrier semaphores. Data moves between devices by JAX's collectives and lax.ppermute only.
A program may use at most 128 MiB of HBM per device.

```python
import jax
import jax.numpy as jnp
from jax import lax

D = 4096
FF = 16384
MICRO = 2
TOK_MB = 80
TOKENS = 320
N_DP = 4


def plant(values, key, smallest, top_value):
    longest = values.shape.index(max(values.shape))
    spots = []
    for shift in (0, 1):
        where = [jax.random.randint(jax.random.fold_in(key, axis), (), 0, length) for axis, length in enumerate(values.shape)]
        where[longest] = (where[longest] + shift) % values.shape[longest]
        spots.append(tuple(where))
    return values.at[spots[0]].set(smallest).at[spots[1]].set(top_value)


def spiked(drawn, stream_key, source, target, shards_of, factor):
    def block_of(axis_at):
        return (jnp.arange(drawn.shape[axis_at]) // (drawn.shape[axis_at] // shards_of)).reshape((-1,) + (1,) * (drawn.ndim - 1 - axis_at))

    near = jax.random.permutation(stream_key, shards_of)[block_of(target)]
    other_side = (block_of(target) + shards_of // 2) % shards_of
    return jnp.where((block_of(source) == near) | (block_of(source) == other_side), factor * drawn, drawn)


def levels(rng, extent, split, smallest, largest):
    gain = 1.0
    for axis_at, blocks in split:
        draws = jax.random.uniform(jax.random.fold_in(jax.random.fold_in(rng, 6), axis_at), (blocks,), jnp.float32, smallest / len(split), largest / len(split))
        gain = gain * jnp.repeat(jnp.exp(draws), extent[axis_at] // blocks).reshape((-1,) + (1,) * (len(extent) - 1 - axis_at))
    return gain


def normal_values(stream_key, shape, scale, limit, cuts=(), kind=jnp.bfloat16):
    level = levels(stream_key, shape, cuts, -0.22, 0.18) if cuts else 1.0
    array = jax.random.normal(stream_key, shape, jnp.float32) * scale * level
    return jnp.minimum(jnp.maximum(array, -limit), limit).astype(kind)


def heavy_noise(rng, shape, spread, reach, split, heavy, held_as=jnp.bfloat16):
    values = spread * jax.random.normal(rng, shape, jnp.float32)
    if split:
        values = values * levels(rng, shape, split, -0.22, 0.18)
    return jnp.clip(spiked(values, jax.random.fold_in(rng, 3), *heavy), -reach, reach).astype(held_as)


def setup_inputs(seed: int = 0) -> dict:
    streams_of = jax.random.split(jax.random.key(seed), 7)
    return {
        "out_grad": heavy_noise(streams_of[0], (MICRO, TOKENS, D), (1.0 / (MICRO * TOKENS) ** 0.5), 0.3125, ((1, 4), (2, 8)), (1, 2, 8, 2.0)),
        "layer_input": heavy_noise(streams_of[1], (MICRO, TOKENS, D), 1.0, 8.0, ((1, 4), (2, 8)), (1, 2, 8, 2.0)),
        "w_down": normal_values(streams_of[2], (FF, D), FF ** -0.5, 0.046875, ((0, 8),)),
        "silu_gate": normal_values(streams_of[3], (MICRO, TOKENS, FF), 1.0, 6.0, ((1, 4), (2, 8))),
        "up_proj": normal_values(streams_of[4], (MICRO, TOKENS, FF), 1.0, 6.0, ((1, 4), (2, 8))),
        "slope_codes": plant(jax.random.randint(streams_of[5], (MICRO, TOKENS // 10, FF), 0, 1073741824), jax.random.fold_in(streams_of[5], 1), 0, 1073741823).astype(jnp.int32),
    }


SLOPE_LEVELS = (-0.09, 0.06, 0.22, 0.41, 0.6, 0.79, 0.96, 1.08)


def decode_slopes(packed):
    shifts = 3 * jnp.arange(10, dtype=jnp.int32)
    pieces = jnp.bitwise_and(jnp.right_shift(packed[..., None, :], shifts[:, None]), 7)
    pieces = pieces.reshape(packed.shape[:-2] + (packed.shape[-2] * 10, packed.shape[-1]))
    result = jnp.full(pieces.shape, SLOPE_LEVELS[0], jnp.float32)
    for symbol in range(1, 8):
        result = jnp.where(pieces == symbol, jnp.float32(SLOPE_LEVELS[symbol]), result)
    return result


def rounded(values):
    return lax.optimization_barrier(values.astype(jnp.bfloat16)).astype(jnp.float32)


def by_group(values):
    columns = values.shape[-1]
    shaped = values.reshape(MICRO, N_DP, TOK_MB, columns).transpose(1, 0, 2, 3)
    return shaped.reshape(N_DP, MICRO * TOK_MB, columns)


def reference(out_grad, layer_input, w_down, silu_gate, up_proj, slope_codes):
    slopes = decode_slopes(slope_codes)
    hidden_grad = jnp.dot(out_grad.reshape(-1, D), w_down.T, preferred_element_type=jnp.float32)
    hidden_grad = hidden_grad.reshape(MICRO, -1, FF)
    gate_act = silu_gate.astype(jnp.float32)
    up_value = up_proj.astype(jnp.float32)
    up_grad = (hidden_grad * gate_act).astype(jnp.bfloat16)
    gate_grad = (hidden_grad * up_value * slopes).astype(jnp.bfloat16)
    hidden = (gate_act * up_value).astype(jnp.bfloat16)

    def add_group(totals, pieces):
        inputs, output_rows, hidden_rows, gate_rows, up_rows = pieces
        gate_part = jnp.dot(inputs.T, gate_rows, preferred_element_type=jnp.float32)
        up_part = jnp.dot(inputs.T, up_rows, preferred_element_type=jnp.float32)
        down_part = jnp.dot(hidden_rows.T, output_rows, preferred_element_type=jnp.float32)
        return (totals[0] + rounded(gate_part), totals[1] + rounded(up_part), totals[2] + rounded(down_part)), None

    start_totals = (jnp.zeros((D, FF), jnp.float32), jnp.zeros((D, FF), jnp.float32), jnp.zeros((FF, D), jnp.float32))
    totals, unused = lax.scan(add_group, start_totals, (by_group(layer_input), by_group(out_grad), by_group(hidden), by_group(gate_grad), by_group(up_grad)))
    return (totals[2].astype(jnp.bfloat16), totals[0].astype(jnp.bfloat16), totals[1].astype(jnp.bfloat16))
```

```python
import functools

import jax
import jax.numpy as jnp
from jax import lax
from jax.experimental import pallas as pl
from jax.experimental.pallas import tpu as pltpu
from jax.sharding import PartitionSpec as P

SLOPE_LEVELS = (-0.09, 0.06, 0.22, 0.41, 0.6, 0.79, 0.96, 1.08)
AXES = ("dp", "tensor")
CORES = 2
CHUNKS = 4


def decode_slopes(packed):
    shifts = 3 * jnp.arange(10, dtype=jnp.int32)
    pieces = jnp.bitwise_and(jnp.right_shift(packed[..., None, :], shifts[:, None]), 7)
    pieces = pieces.reshape(packed.shape[:-2] + (packed.shape[-2] * 10, packed.shape[-1]))
    result = jnp.full(pieces.shape, SLOPE_LEVELS[0], jnp.float32)
    for symbol in range(1, 8):
        result = jnp.where(pieces == symbol, jnp.float32(SLOPE_LEVELS[symbol]), result)
    return result


def hidden_grads(pieces, w_down, scaled_up, gate_act, place, chunk, chunk_width, block):
    rows, part = pieces[0].shape
    count = len(pieces)
    width = w_down.shape[1]
    steps = chunk_width // block

    def body(place_ref, *refs):
        piece_refs, (w_ref, up_ref, gate_ref, out_ref) = refs[:count], refs[count:]
        total = jnp.zeros((rows, block), jnp.float32)
        for m in range(count):
            at = pl.multiple_of(jnp.bitwise_xor(place_ref[0], m) * part, part)
            total += lax.dot_general(
                piece_refs[m][...],
                w_ref[:, pl.ds(at, part)],
                (((1,), (1,)), ((), ())),
                preferred_element_type=jnp.float32,
            )
        out_ref[0] = (total * up_ref[...]).astype(jnp.bfloat16)
        out_ref[1] = (total * gate_ref[...].astype(jnp.float32)).astype(jnp.bfloat16)

    column = pl.BlockSpec((rows, block), lambda i, s: (0, chunk * steps + i))
    return pl.pallas_call(
        body,
        grid_spec=pltpu.PrefetchScalarGridSpec(
            num_scalar_prefetch=1,
            grid=(steps,),
            in_specs=[pl.BlockSpec((rows, part), lambda i, s: (0, 0))] * count
            + [pl.BlockSpec((block, width), lambda i, s: (chunk * steps + i, 0)), column, column],
            out_specs=pl.BlockSpec((2, rows, block), lambda i, s: (0, 0, i)),
        ),
        out_shape=jax.ShapeDtypeStruct((2, rows, chunk_width), jnp.bfloat16),
        cost_estimate=pl.CostEstimate(
            flops=2 * rows * width * chunk_width, bytes_accessed=2 * width * chunk_width, transcendentals=0
        ),
        name="hidden_grads",
    )(place, *pieces, w_down, scaled_up, gate_act)


def own_blocks(pieces, place, per_block):
    rows, part = pieces[0].shape
    count = len(pieces)

    def body(place_ref, *refs):
        out_ref = refs[count]
        for m in range(count):
            spot = jnp.bitwise_xor(place_ref[0], m) - place_ref[1]
            for c in range(CORES):
                for j in range(per_block):

                    @pl.when(spot == c * per_block + j)
                    def _():
                        out_ref[c, :, j * part : (j + 1) * part] = refs[m][...]

    return pl.pallas_call(
        body,
        grid_spec=pltpu.PrefetchScalarGridSpec(
            num_scalar_prefetch=1,
            grid=(1,),
            in_specs=[pl.BlockSpec((rows, part), lambda i, s: (0, 0))] * count,
            out_specs=pl.BlockSpec((CORES, rows, per_block * part), lambda i, s: (0, 0, 0)),
        ),
        out_shape=jax.ShapeDtypeStruct((CORES, rows, per_block * part), jnp.bfloat16),
        name="own_blocks",
    )(place, *pieces)


def transposed_rows(pieces, order):
    rows = sum(group[0].shape[0] for group in pieces)
    parts = len(pieces[0])
    part = pieces[0][0].shape[1]
    flat = [group[j] for j in range(parts) for group in pieces]
    count = len(flat)

    def body(order_ref, *refs):
        out_ref = refs[count]
        for j in range(parts):
            values = jnp.concatenate([refs[j * len(pieces) + i][...] for i in range(len(pieces))], axis=0)
            at = pl.multiple_of(jnp.bitwise_xor(order_ref[0], j) * part, part)
            out_ref[pl.ds(at, part), :] = values.T

    return pl.pallas_call(
        body,
        grid_spec=pltpu.PrefetchScalarGridSpec(
            num_scalar_prefetch=1,
            grid=(1,),
            in_specs=[pl.BlockSpec(a.shape, lambda i, s: (0, 0)) for a in flat],
            out_specs=pl.BlockSpec((parts * part, rows), lambda i, s: (0, 0)),
        ),
        out_shape=jax.ShapeDtypeStruct((parts * part, rows), jnp.bfloat16),
        name="transposed_rows",
    )(order, *flat)


def down_grad(hidden, outputs, block):
    count, outs = len(hidden), len(outputs)
    hidden_width = hidden[0].shape[1]
    width = outputs[0].shape[1]
    rows = sum(a.shape[0] for a in hidden)

    def body(*refs):
        left = jnp.concatenate([r[...] for r in refs[:count]], axis=0)
        right = jnp.concatenate([r[...] for r in refs[count : count + outs]], axis=0)
        refs[-1][...] = lax.dot_general(
            left, right, (((0,), (0,)), ((), ())), preferred_element_type=jnp.float32
        ).astype(jnp.bfloat16)

    return pl.pallas_call(
        body,
        grid=(hidden_width // block,),
        in_specs=[pl.BlockSpec((a.shape[0], block), lambda i: (0, i)) for a in hidden]
        + [pl.BlockSpec(a.shape, lambda i: (0, 0)) for a in outputs],
        out_specs=pl.BlockSpec((block, width), lambda i: (i, 0)),
        out_shape=jax.ShapeDtypeStruct((hidden_width, width), jnp.bfloat16),
        cost_estimate=pl.CostEstimate(
            flops=2 * rows * hidden_width * width, bytes_accessed=2 * width * hidden_width, transcendentals=0
        ),
        name="down_grad",
    )(*hidden, *outputs)


def gate_up_grad(inputs_t, grads, carried, chunk, hidden_width, block):
    count = len(grads)
    width, rows = inputs_t.shape
    chunk_width = grads[0].shape[2]
    extra = len(carried)

    def body(left_ref, *refs):
        grad_refs, outs = refs[:count], refs[count + extra :]
        for k in range(2):
            right = jnp.concatenate([r[k] for r in grad_refs], axis=0)
            outs[k][...] = lax.dot_general(
                left_ref[...], right, (((1,), (0,)), ((), ())), preferred_element_type=jnp.float32
            ).astype(jnp.bfloat16)

    return pl.pallas_call(
        body,
        grid=(width // block,),
        in_specs=[pl.BlockSpec((block, rows), lambda i: (i, 0))]
        + [pl.BlockSpec(a.shape, lambda i: (0, 0, 0)) for a in grads]
        + [pl.BlockSpec(memory_space=pl.ANY)] * extra,
        out_specs=[pl.BlockSpec((block, chunk_width), lambda i: (i, chunk))] * 2,
        out_shape=[jax.ShapeDtypeStruct((width, hidden_width), jnp.bfloat16)] * 2,
        input_output_aliases={1 + count + k: k for k in range(extra)},
        cost_estimate=pl.CostEstimate(
            flops=4 * rows * chunk_width * width, bytes_accessed=4 * width * chunk_width, transcendentals=0
        ),
        name="gate_up_grad",
    )(inputs_t, *grads, *carried)


def shards(groups, places, out_grad, layer_input, w_down, silu_gate, up_proj, slope_codes):
    chips = groups // CORES
    per_block = places // groups
    hidden_width = w_down.shape[0]
    group, place = lax.axis_index("dp"), lax.axis_index("tensor")
    chunk_width = hidden_width // CHUNKS
    everyone = [(g, t) for g in range(groups) for t in range(places)]

    def send(values, target):
        pairs = []
        for g, t in everyone:
            to = target(g, t)
            if to is not None:
                pairs.append((g * places + t, to[0] * places + to[1]))
        return lax.ppermute(values, AXES, pairs)

    def other_core(values):
        return send(values, lambda g, t: (g ^ 1, t))

    def from_chip(values, k):
        return send(values, lambda g, t: ((g - CORES * k) % groups, t))

    def flip(values, bit):
        return send(values, lambda g, t: (g, t ^ bit))

    def to_owner(values, k):
        def target(g, t):
            owner = t // per_block // CORES
            return (owner * CORES + g % CORES, t) if g // CORES == (owner + k) % chips and k else None

        return send(values, target)

    def spread(values):
        bit = places // 2
        while bit >= per_block:
            low = bit * 2 - 1

            def target(g, t, bit=bit, low=low):
                home = g * per_block
                return (g, t ^ bit) if (t & low) // per_block == (home & low) // per_block else None

            received = send(values, target)
            home = group * per_block
            here = (place & low) // per_block == (home & low) // per_block
            values = jnp.where(here, values, received)
            bit //= 2
        parts = {0: values}
        for m in range(1, per_block):
            parts[m] = flip(parts[m & (m - 1)], m & -m)
        return [parts[m] for m in range(per_block)]

    out_rows = out_grad.reshape(-1, out_grad.shape[2])
    in_rows = layer_input.reshape(-1, layer_input.shape[2])
    gate_act = silu_gate.reshape(-1, hidden_width)
    up_value = up_proj.reshape(-1, hidden_width)

    pieces = {0: out_rows}
    for m in range(1, places):
        pieces[m] = flip(pieces[m & (m - 1)], m & -m)
    pieces = [pieces[m] for m in range(places)]

    hidden = (gate_act.astype(jnp.float32) * up_value.astype(jnp.float32)).astype(jnp.bfloat16)

    def all_groups(values):
        found = [values, other_core(values)]
        for k in range(1, chips):
            received = from_chip(values, k)
            found += [received, other_core(received)]
        return found

    in_crossed = [to_owner(in_rows, k) for k in range(1, chips)]
    out_crossed = [to_owner(out_rows, k) for k in range(1, chips)]
    hidden_all = all_groups(hidden)

    def both_cores(values):
        return spread(jnp.concatenate([values, other_core(values)], axis=0))

    in_blocks = [both_cores(values) for values in [in_rows] + in_crossed]
    out_blocks = [both_cores(values) for values in out_crossed]

    slopes = decode_slopes(slope_codes).reshape(-1, hidden_width)
    scaled_up = up_value.astype(jnp.float32) * slopes
    spot = place.astype(jnp.int32)[None]
    low = (place % per_block).astype(jnp.int32)[None]

    grads = [
        hidden_grads(pieces, w_down, scaled_up, gate_act, spot, i, chunk_width, min(256, chunk_width))
        for i in range(CHUNKS)
    ]
    first = (group // CORES * CORES * per_block).astype(jnp.int32)
    mine = own_blocks(pieces, jnp.stack([spot[0], first]), per_block)
    core = group % CORES
    kept = lax.dynamic_index_in_dim(mine, core, 0, keepdims=False)
    given = lax.dynamic_index_in_dim(mine, 1 - core, 0, keepdims=False)
    out_all = [kept, other_core(given)]
    for parts in out_blocks:
        ordered = [
            functools.reduce(lambda a, m: jnp.where(low[0] == (j ^ m), parts[m], a), range(1, per_block), parts[0])
            for j in range(per_block)
        ]
        out_all.append(jnp.concatenate(ordered, axis=1))
    grad_down = down_grad(hidden_all, out_all, min(256, hidden_width))

    inputs_t = transposed_rows(in_blocks, low)
    carried = []
    for i in range(CHUNKS):
        carried = gate_up_grad(
            inputs_t, all_groups(grads[i]), carried, i, hidden_width, min(256, inputs_t.shape[0])
        )
    return (grad_down, carried[0], carried[1])


def solution(mesh):
    return jax.shard_map(
        functools.partial(shards, mesh.shape["dp"], mesh.shape["tensor"]),
        mesh=mesh,
        in_specs=(
            P(None, "dp", "tensor"),
            P(None, "dp", "tensor"),
            P("tensor", None),
            P(None, "dp", "tensor"),
            P(None, "dp", "tensor"),
            P(None, "dp", "tensor"),
        ),
        out_specs=(P("tensor", "dp"), P("dp", "tensor"), P("dp", "tensor")),
        check_vma=False,
    )
```

```python
import functools

import jax
import jax.numpy as jnp
from jax import lax
from jax.experimental import pallas as pl
from jax.experimental.pallas import tpu as pltpu
from jax.sharding import PartitionSpec as P

SLOPE_LEVELS = (-0.09, 0.06, 0.22, 0.41, 0.6, 0.79, 0.96, 1.08)
AXES = ("dp", "tensor")
CORES = 2
CHUNKS = 2


def decode_slopes(packed):
    shifts = 3 * jnp.arange(10, dtype=jnp.int32)
    pieces = jnp.bitwise_and(jnp.right_shift(packed[..., None, :], shifts[:, None]), 7)
    pieces = pieces.reshape(packed.shape[:-2] + (packed.shape[-2] * 10, packed.shape[-1]))
    result = jnp.full(pieces.shape, SLOPE_LEVELS[0], jnp.float32)
    for symbol in range(1, 8):
        result = jnp.where(pieces == symbol, jnp.float32(SLOPE_LEVELS[symbol]), result)
    return result


def whole_block(shape):
    return pl.BlockSpec(shape, lambda *_: (0,) * len(shape))


def hidden_part(pieces, masks, w_down, where, total, chunk, chunk_width, block, finish, blocks):
    rows, part = pieces[0].shape
    count = len(pieces)
    steps = chunk_width // block
    per_block = blocks
    inputs = list(pieces) + [w_down] * count
    in_specs = [whole_block((rows, part))] * count
    in_specs += [
        pl.BlockSpec((block, part), lambda i, s, m=m: (chunk * steps + i, jnp.bitwise_xor(s[0], m))) for m in masks
    ]
    if total is not None:
        inputs.append(total)
        in_specs.append(pl.BlockSpec((block, rows), lambda i, s: (chunk * steps + i, 0)))
    if finish:
        inputs += finish
        in_specs += [pl.BlockSpec((rows, block), lambda i, s: (0, chunk * steps + i))] * 2
        out_shape = [jax.ShapeDtypeStruct((2, rows, chunk_width), jnp.bfloat16)]
        out_specs = [pl.BlockSpec((2, rows, block), lambda i, s: (0, 0, i))]
    else:
        out_shape = [jax.ShapeDtypeStruct((chunk_width, rows), jnp.float32)]
        out_specs = [pl.BlockSpec((block, rows), lambda i, s: (i, 0))]
    if per_block:
        out_shape += [jax.ShapeDtypeStruct((rows, part), jnp.bfloat16)] * 2
        out_specs += [whole_block((rows, part))] * 2

    def body(where_ref, *refs):
        ins, outs = refs[: len(inputs)], refs[len(inputs) :]
        found = ins[2 * count][...] if total is not None else None
        for m in range(count):
            product = lax.dot_general(
                ins[count + m][...], ins[m][...], (((1,), (1,)), ((), ())), preferred_element_type=jnp.float32
            )
            found = product if found is None else found + product
        if finish:
            up_ref, gate_ref = ins[-2:]
            found = found.T
            outs[0][0] = (found * up_ref[...]).astype(jnp.bfloat16)
            outs[0][1] = (found * gate_ref[...].astype(jnp.float32)).astype(jnp.bfloat16)
        else:
            outs[0][...] = found
        if per_block:

            @pl.when(pl.program_id(0) == 0)
            def _():
                for m in range(count):
                    owner = jnp.bitwise_xor(where_ref[0], masks[m]) // per_block
                    for c in range(CORES):

                        @pl.when(owner == jnp.bitwise_xor(where_ref[1], c))
                        def _():
                            outs[1 + c][...] = ins[m][...]

    width = part * count
    return pl.pallas_call(
        body,
        grid_spec=pltpu.PrefetchScalarGridSpec(
            num_scalar_prefetch=1, grid=(steps,), in_specs=in_specs, out_specs=out_specs
        ),
        out_shape=out_shape,
        cost_estimate=pl.CostEstimate(
            flops=2 * rows * width * chunk_width, bytes_accessed=2 * width * chunk_width, transcendentals=0
        ),
        name="hidden_part",
    )(where, *inputs)


def down_grad(hidden, outputs, low, block):
    count, parts = len(hidden), len(outputs)
    hidden_width = hidden[0].shape[1]
    part = outputs[0][0].shape[1]
    width = parts * part
    rows = sum(a.shape[0] for a in hidden)
    flat = [a for group in outputs for a in group]

    def body(low_ref, *refs):
        lefts, rights, out_ref, right_ref = refs[:count], refs[count:-2], refs[-2], refs[-1]

        @pl.when(pl.program_id(0) == 0)
        def _():
            for j in range(parts):
                group = rights[j * len(rights) // parts : (j + 1) * len(rights) // parts]
                at = pl.multiple_of(jnp.bitwise_xor(low_ref[0], j) * part, part)
                start = 0
                for r in group:
                    right_ref[start : start + r.shape[0], pl.ds(at, part)] = r[...]
                    start += r.shape[0]

        left = jnp.concatenate([r[...] for r in lefts], axis=0)
        out_ref[...] = lax.dot_general(
            left, right_ref[...], (((0,), (0,)), ((), ())), preferred_element_type=jnp.float32
        ).astype(jnp.bfloat16)

    return pl.pallas_call(
        body,
        grid_spec=pltpu.PrefetchScalarGridSpec(
            num_scalar_prefetch=1,
            grid=(hidden_width // block,),
            in_specs=[pl.BlockSpec((a.shape[0], block), lambda i, s: (0, i)) for a in hidden]
            + [whole_block(a.shape) for a in flat],
            out_specs=pl.BlockSpec((block, width), lambda i, s: (i, 0)),
            scratch_shapes=[pltpu.VMEM((rows, width), jnp.bfloat16)],
        ),
        out_shape=jax.ShapeDtypeStruct((hidden_width, width), jnp.bfloat16),
        cost_estimate=pl.CostEstimate(
            flops=2 * rows * hidden_width * width, bytes_accessed=2 * width * hidden_width, transcendentals=0
        ),
        name="down_grad",
    )(low, *hidden, *flat)


def gate_up_grad(inputs, grads, low, carried, chunk, hidden_width, block):
    count, parts = len(grads), len(inputs)
    rows, part = inputs[0].shape
    width = parts * part
    chunk_width = grads[0].shape[2]
    steps = chunk_width // block
    extra = len(carried)

    def body(low_ref, *refs):
        in_refs, grad_refs = refs[:parts], refs[parts : parts + count]
        outs, left_ref = refs[-3:-1], refs[-1]

        @pl.when(pl.program_id(0) == 0)
        def _():
            for j in range(parts):
                at = pl.multiple_of(jnp.bitwise_xor(low_ref[0], j) * part, part)
                left_ref[pl.ds(at, part), :] = in_refs[j][...].T

        for k in range(2):
            right = jnp.concatenate([r[k] for r in grad_refs], axis=0)
            outs[k][...] = lax.dot_general(
                left_ref[...], right, (((1,), (0,)), ((), ())), preferred_element_type=jnp.float32
            ).astype(jnp.bfloat16)

    return pl.pallas_call(
        body,
        grid_spec=pltpu.PrefetchScalarGridSpec(
            num_scalar_prefetch=1,
            grid=(steps,),
            in_specs=[whole_block(a.shape) for a in inputs]
            + [pl.BlockSpec(a.shape[:2] + (block,), lambda i, s: (0, 0, i)) for a in grads]
            + [pl.BlockSpec(memory_space=pl.ANY)] * extra,
            out_specs=[pl.BlockSpec((width, block), lambda i, s: (0, chunk * steps + i))] * 2,
            scratch_shapes=[pltpu.VMEM((width, rows), jnp.bfloat16)],
        ),
        out_shape=[jax.ShapeDtypeStruct((width, hidden_width), jnp.bfloat16)] * 2,
        input_output_aliases={1 + parts + count + k: k for k in range(extra)},
        cost_estimate=pl.CostEstimate(
            flops=4 * rows * chunk_width * width, bytes_accessed=4 * width * chunk_width, transcendentals=0
        ),
        name="gate_up_grad",
    )(low, *inputs, *grads, *carried)


def shards(groups, places, out_grad, layer_input, w_down, silu_gate, up_proj, slope_codes):
    chips = groups // CORES
    per_block = places // groups
    per_chip = per_block * CORES
    hidden_width = w_down.shape[0]
    group, place = lax.axis_index("dp"), lax.axis_index("tensor")
    chunk_width = hidden_width // CHUNKS
    everyone = [(g, t) for g in range(groups) for t in range(places)]

    def send(values, target):
        pairs = []
        for g, t in everyone:
            to = target(g, t)
            if to is not None:
                pairs.append((g * places + t, to[0] * places + to[1]))
        return lax.ppermute(values, AXES, pairs)

    def other_core(values):
        return send(values, lambda g, t: (g ^ 1, t))

    def from_chip(values, k):
        return send(values, lambda g, t: ((g - CORES * k) % groups, t))

    def flip(values, bits):
        return send(values, lambda g, t: (g, t ^ bits))

    out_rows = out_grad.reshape(-1, out_grad.shape[2])
    in_rows = layer_input.reshape(-1, layer_input.shape[2])
    gate_act = silu_gate.reshape(-1, hidden_width)
    up_value = up_proj.reshape(-1, hidden_width)
    rows = out_rows.shape[0]

    pieces = {0: out_rows}
    for m in range(places - per_chip, 0, -per_chip):
        pieces[m] = flip(out_rows, m)
    for m in range(per_block, places, per_block):
        if m not in pieces:
            pieces[m] = flip(out_rows, m)
    for m in range(1, per_block):
        pieces[m] = flip(out_rows, m)
    crossing = {0: in_rows}
    for m in range(places - per_chip, 0, -per_chip):
        crossing[m] = flip(in_rows, m)
    for m in range(places):
        if m not in pieces:
            pieces[m] = flip(pieces[m - m % per_block], m % per_block)

    hidden = (gate_act.astype(jnp.float32) * up_value.astype(jnp.float32)).astype(jnp.bfloat16)

    def all_groups(values):
        found = [values, other_core(values)]
        for k in range(1, chips):
            received = from_chip(values, k)
            found += [received, other_core(received)]
        return found

    hidden_all = all_groups(hidden)

    def owned_by(held, chip):
        found = held[0]
        for m in range(per_chip, places, per_chip):
            found = jnp.where((place ^ m) // per_chip == chip, held[m], found)
        return found

    chip = group // CORES
    mine = owned_by(crossing, chip)
    in_held = [mine, other_core(mine)]
    out_held = []
    for k in range(1, chips):
        target = (chip - k) % chips
        crossed = from_chip(jnp.concatenate([owned_by(crossing, target), owned_by(pieces, target)], axis=0), k)
        for values in (crossed, other_core(crossed)):
            in_held.append(values[:rows])
            out_held.append(values[rows:])
    holds = (place // per_block) % CORES == group % CORES

    def to_blocks(held):
        held = jnp.concatenate(held, axis=0)
        received = send(
            held, lambda g, t: (g, t ^ per_block) if (t // per_block) % CORES == g % CORES else None
        )
        held = jnp.where(holds, held, received)
        return [held] + [flip(held, j) for j in range(1, per_block)]

    in_blocks = to_blocks(in_held)
    out_blocks = to_blocks(out_held)

    slopes = decode_slopes(slope_codes).reshape(-1, hidden_width)
    scaled_up = up_value.astype(jnp.float32) * slopes
    where = jnp.stack([place, group]).astype(jnp.int32)
    low = (place % per_block).astype(jnp.int32)[None]

    block = min(512, chunk_width)
    total = None
    outputs = []
    for j in range(per_block):
        masks = list(range(j, places, per_block))
        part = [pieces[m] for m in masks]
        if j < per_block - 1:
            total, kept, given = hidden_part(part, masks, w_down, where, total, 0, hidden_width, block, None, per_block)
        else:
            grads = []
            for i in range(CHUNKS):
                found = hidden_part(
                    part, masks, w_down, where, total, i, chunk_width, block, [scaled_up, gate_act],
                    0 if i else per_block,
                )
                grads.append(found[0])
                if not i:
                    kept, given = found[1:]
        outputs.append([kept, other_core(given)] + [out_blocks[j]])
    grads_all = [all_groups(values) for values in grads]
    grad_down = down_grad(hidden_all, outputs, low, min(1024, hidden_width))

    carried = []
    for i in range(CHUNKS):
        carried = gate_up_grad(in_blocks, grads_all[i], low, carried, i, hidden_width, block)
    return (grad_down, carried[0], carried[1])


def solution(mesh):
    return jax.shard_map(
        functools.partial(shards, mesh.shape["dp"], mesh.shape["tensor"]),
        mesh=mesh,
        in_specs=(
            P(None, "dp", "tensor"),
            P(None, "dp", "tensor"),
            P("tensor", None),
            P(None, "dp", "tensor"),
            P(None, "dp", "tensor"),
            P(None, "dp", "tensor"),
        ),
        out_specs=(P("tensor", "dp"), P("dp", "tensor"), P("dp", "tensor")),
        check_vma=False,
    )
```

```python
import functools

import jax
import jax.numpy as jnp
from jax import lax
from jax.experimental import pallas as pl
from jax.experimental.pallas import tpu as pltpu
from jax.sharding import PartitionSpec as P


SLOPE_LEVELS = (-0.09, 0.06, 0.22, 0.41, 0.6, 0.79, 0.96, 1.08)
AXES = ("dp", "tensor")
CORES = 2
EIGHTHS = (4, 4)
VMEM_LIMIT = 20
LANES = 128
DOWN_PARTS = 2
DOWN_BLOCK = 512


IN_VMEM = pl.BlockSpec(memory_space=pltpu.VMEM)
IN_HBM = pl.BlockSpec(memory_space=pltpu.HBM)
PARAMS = pltpu.CompilerParams(vmem_limit_bytes=VMEM_LIMIT << 20)


def first_half(place, group, w_down, gate_act, up_value):
    rows, hidden_width = up_value.shape
    half = w_down.shape[0] // 2

    def body(place_ref, group_ref, w_ref, gate_ref, up_ref, w_out, hidden_ref, gate_buf, up_buf, done):
        copies = [
            pltpu.make_async_copy(gate_ref, gate_buf, done.at[0]),
            pltpu.make_async_copy(up_ref, up_buf, done.at[1]),
            pltpu.make_async_copy(w_ref.at[pl.ds(0, half)], w_out.at[pl.ds(0, half)], done.at[2]),
        ]
        for copy in copies:
            copy.start()
        for copy in copies[:2]:
            copy.wait()
        hidden_ref[...] = (gate_buf[...].astype(jnp.float32) * up_buf[...].astype(jnp.float32)).astype(jnp.bfloat16)
        copies[2].wait()

    return pl.pallas_call(
        body,
        grid_spec=pltpu.PrefetchScalarGridSpec(
            num_scalar_prefetch=2,
            grid=(1,),
            in_specs=[IN_HBM] * 3,
            out_specs=[IN_VMEM] * 2,
            scratch_shapes=[pltpu.VMEM((rows, hidden_width), jnp.bfloat16)] * 2 + [pltpu.SemaphoreType.DMA((3,))],
        ),
        out_shape=[
            jax.ShapeDtypeStruct(w_down.shape, jnp.bfloat16),
            jax.ShapeDtypeStruct((rows, hidden_width), jnp.bfloat16),
        ],
        compiler_params=PARAMS,
        cost_estimate=pl.CostEstimate(flops=rows * hidden_width, bytes_accessed=2 * w_down.size, transcendentals=0),
        name="first_half",
    )(place, group, w_down, gate_act, up_value)


def second_half(w_down, up_value, codes, w_here):
    micro, words, hidden_width = codes.shape
    rows = up_value.shape[0]
    per_word = rows // (micro * words)
    half = w_down.shape[0] // 2

    def body(w_ref, up_ref, code_ref, held_ref, w_out, scaled_ref, up_buf, code_buf, level_ref, done):
        copies = [
            pltpu.make_async_copy(code_ref, code_buf, done.at[0]),
            pltpu.make_async_copy(up_ref, up_buf, done.at[1]),
            pltpu.make_async_copy(w_ref.at[pl.ds(half, half)], w_out.at[pl.ds(half, half)], done.at[2]),
        ]
        for copy in copies:
            copy.start()
        for copy in copies[:2]:
            copy.wait()

        def columns(n, carry):
            here = pl.ds(pl.multiple_of(n * LANES, LANES), LANES)
            for m in range(micro):
                packed = code_buf[m, :, here]
                for k in range(per_word):
                    piece = jnp.bitwise_and(jnp.right_shift(packed, 3 * k), 7)
                    level = jnp.full(piece.shape, SLOPE_LEVELS[0], jnp.float32)
                    for symbol in range(1, 8):
                        level = jnp.where(piece == symbol, jnp.float32(SLOPE_LEVELS[symbol]), level)
                    level_ref[pl.ds(m * words * per_word + k, words, per_word), :] = level
            scaled_ref[:, here] = up_buf[:, here].astype(jnp.float32) * level_ref[...]
            return carry

        lax.fori_loop(0, hidden_width // LANES, columns, 0)
        copies[2].wait()

    return pl.pallas_call(
        body,
        in_specs=[IN_HBM] * 3 + [IN_VMEM],
        out_specs=[IN_VMEM] * 2,
        out_shape=[
            jax.ShapeDtypeStruct(w_down.shape, jnp.bfloat16),
            jax.ShapeDtypeStruct((rows, hidden_width), jnp.float32),
        ],
        scratch_shapes=[
            pltpu.VMEM((rows, hidden_width), jnp.bfloat16),
            pltpu.VMEM(codes.shape, jnp.int32),
            pltpu.VMEM((rows, LANES), jnp.float32),
            pltpu.SemaphoreType.DMA((3,)),
        ],
        input_output_aliases={3: 0},
        compiler_params=PARAMS,
        cost_estimate=pl.CostEstimate(flops=rows * hidden_width, bytes_accessed=2 * w_down.size, transcendentals=0),
        name="second_half",
    )(w_down, up_value, codes, w_here)


def arrange(place, group, inputs, rows, blocks, moves):
    width = inputs[0].shape[1]

    def body(place_ref, group_ref, *refs):
        sources, targets = refs[: len(inputs)], refs[len(inputs) :]
        for target, at, source, start, condition in moves:

            def copy(target=target, at=at, source=source, start=start):
                values = sources[source][start * rows : (start + 1) * rows, :]
                targets[target][at * rows : (at + 1) * rows, :] = values

            if condition is None:
                copy()
            else:
                pl.when(condition(place_ref[0], group_ref[0]))(copy)

    return pl.pallas_call(
        body,
        grid_spec=pltpu.PrefetchScalarGridSpec(
            num_scalar_prefetch=2,
            grid=(1,),
            in_specs=[IN_VMEM] * len(inputs),
            out_specs=[IN_VMEM] * len(blocks),
        ),
        out_shape=[jax.ShapeDtypeStruct((count * rows, width), jnp.bfloat16) for count in blocks],
        compiler_params=PARAMS,
        cost_estimate=pl.CostEstimate(flops=rows * width, bytes_accessed=4 * rows * width, transcendentals=0),
    )(place, group, *inputs)


def hidden_grads(pieces, w_down, place, group, scaled_up, gate_act, begin, chunk_width, block, per_block):
    rows, part = pieces[0].shape
    count = len(pieces)
    width = part * count
    out_shape = [jax.ShapeDtypeStruct((2, rows, chunk_width), jnp.bfloat16)]
    if per_block:
        out_shape += [jax.ShapeDtypeStruct((per_block * rows, part), jnp.bfloat16)] * CORES

    def body(place_ref, group_ref, *refs):
        piece_refs, (w_ref, up_ref, gate_ref), outs = refs[:count], refs[count : count + 3], refs[count + 3 :]
        step = pl.program_id(0)
        here = pl.ds(pl.multiple_of(begin + step * block, block), block)
        there = pl.ds(pl.multiple_of(step * block, block), block)
        found = None
        for m in range(count):
            at = pl.multiple_of(jnp.bitwise_xor(place_ref[0], m) * part, part)
            product = lax.dot_general(
                w_ref[here, pl.ds(at, part)], piece_refs[m][...], (((1,), (1,)), ((), ())),
                preferred_element_type=jnp.float32,
            )
            found = product if found is None else found + product
        found = found.T
        outs[0][0, :, there] = (found * up_ref[:, here]).astype(jnp.bfloat16)
        outs[0][1, :, there] = (found * gate_ref[:, here].astype(jnp.float32)).astype(jnp.bfloat16)
        if per_block:

            @pl.when(step == 0)
            def _():
                for m in range(count):
                    owner = jnp.bitwise_xor(place_ref[0], m) // per_block
                    j = m % per_block
                    for c in range(CORES):

                        @pl.when(owner == jnp.bitwise_xor(group_ref[0], c))
                        def _():
                            outs[1 + c][j * rows : (j + 1) * rows, :] = piece_refs[m][...]

    return pl.pallas_call(
        body,
        grid_spec=pltpu.PrefetchScalarGridSpec(
            num_scalar_prefetch=2,
            grid=(chunk_width // block,),
            in_specs=[IN_VMEM] * (count + 3),
            out_specs=[IN_VMEM] * len(out_shape),
        ),
        out_shape=out_shape,
        compiler_params=PARAMS,
        cost_estimate=pl.CostEstimate(
            flops=2 * rows * width * chunk_width, bytes_accessed=2 * width * chunk_width, transcendentals=0
        ),
        name="hidden_grads",
    )(place, group, *pieces, w_down, scaled_up, gate_act)


def flattened(groups):
    flat = [item for group in groups for item in group]
    return [a for a, n in flat], [n for a, n in flat]


def down_grad(hidden, outputs, rows, place, carried, begin, size, block):
    count, parts = len(hidden), len(outputs)
    hidden_width = hidden[0].shape[1]
    part = outputs[0][0][0].shape[1]
    width = parts * part
    tokens = rows * count
    flat, spots = flattened(outputs)

    def body(place_ref, *refs):
        lefts, rights, out_ref, right_ref = refs[:count], refs[count : count + len(flat)], refs[-2], refs[-1]

        @pl.when(pl.program_id(0) == 0)
        def _():
            for j in range(parts):
                at = pl.multiple_of(jnp.bitwise_xor(lax.rem(place_ref[0], parts), j) * part, part)
                for n in range(count):
                    values = rights[j * count + n][pl.ds(spots[j * count + n] * rows, rows), :]
                    right_ref[n * rows : (n + 1) * rows, pl.ds(at, part)] = values

        here = pl.ds(pl.multiple_of(begin + pl.program_id(0) * block, block), block)
        left = jnp.concatenate([r[:, here] for r in lefts], axis=0)
        out_ref[...] = lax.dot_general(
            left, right_ref[...], (((0,), (0,)), ((), ())), preferred_element_type=jnp.float32
        ).astype(jnp.bfloat16)

    return pl.pallas_call(
        body,
        grid_spec=pltpu.PrefetchScalarGridSpec(
            num_scalar_prefetch=1,
            grid=(size // block,),
            in_specs=[IN_VMEM] * (count + len(flat)) + [pl.BlockSpec(memory_space=pl.ANY)] * len(carried),
            out_specs=pl.BlockSpec((block, width), lambda i, s: (begin // block + i, 0)),
            scratch_shapes=[pltpu.VMEM((tokens, width), jnp.bfloat16)],
        ),
        out_shape=jax.ShapeDtypeStruct((hidden_width, width), jnp.bfloat16),
        cost_estimate=pl.CostEstimate(
            flops=2 * tokens * size * width, bytes_accessed=2 * width * size, transcendentals=0
        ),
        input_output_aliases={1 + count + len(flat): 0} if carried else {},
        compiler_params=PARAMS,
        name="down_grad",
    )(place, *hidden, *flat, *carried)


def gate_up_grad(inputs, grads, rows, place, carried, begin, hidden_width, block):
    count, parts = len(grads), len(inputs)
    part = inputs[0][0][0].shape[1]
    tokens = rows * count
    width = parts * part
    chunk_width = grads[0].shape[2]
    steps, first = chunk_width // block, begin // block
    extra = len(carried)
    flat, spots = flattened(inputs)

    def body(place_ref, *refs):
        in_refs, grad_refs = refs[: parts * count], refs[parts * count : (parts + 1) * count]
        outs, left_ref = refs[-3:-1], refs[-1]

        @pl.when(pl.program_id(0) == 0)
        def _():
            for j in range(parts):
                at = pl.multiple_of(jnp.bitwise_xor(lax.rem(place_ref[0], parts), j) * part, part)
                values = jnp.concatenate(
                    [in_refs[n][pl.ds(spots[n] * rows, rows), :] for n in range(j * count, (j + 1) * count)], axis=0
                )
                left_ref[pl.ds(at, part), :] = values.T

        here = pl.ds(pl.multiple_of(pl.program_id(0) * block, block), block)
        for k in range(2):
            right = jnp.concatenate([r[k, :, here] for r in grad_refs], axis=0)
            outs[k][...] = lax.dot_general(
                left_ref[...], right, (((1,), (0,)), ((), ())), preferred_element_type=jnp.float32
            ).astype(jnp.bfloat16)

    return pl.pallas_call(
        body,
        grid_spec=pltpu.PrefetchScalarGridSpec(
            num_scalar_prefetch=1,
            grid=(steps,),
            in_specs=[IN_VMEM] * (len(flat) + count) + [pl.BlockSpec(memory_space=pl.ANY)] * extra,
            out_specs=[pl.BlockSpec((width, block), lambda i, s: (0, first + i))] * 2,
            scratch_shapes=[pltpu.VMEM((width, tokens), jnp.bfloat16)],
        ),
        out_shape=[jax.ShapeDtypeStruct((width, hidden_width), jnp.bfloat16)] * 2,
        input_output_aliases={1 + (parts + 1) * count + k: k for k in range(extra)},
        cost_estimate=pl.CostEstimate(
            flops=4 * tokens * chunk_width * width, bytes_accessed=4 * width * chunk_width, transcendentals=0
        ),
        compiler_params=PARAMS,
        name="gate_up_grad",
    )(place, *flat, *grads, *carried)


def shards(groups, places, out_grad, layer_input, w_down, silu_gate, up_proj, slope_codes):
    chips = groups // CORES
    per_block = places // groups
    per_chip = per_block * CORES
    hidden_width = w_down.shape[0]
    group, place = lax.axis_index("dp"), lax.axis_index("tensor")
    everyone = [(g, t) for g in range(groups) for t in range(places)]

    def send(values, target):
        pairs = []
        for g, t in everyone:
            to = target(g, t)
            if to is not None:
                pairs.append((g * places + t, to[0] * places + to[1]))
        return lax.ppermute(values, AXES, pairs)

    def other_core(values):
        return send(values, lambda g, t: (g ^ 1, t))

    def from_chip(values, k):
        return send(values, lambda g, t: ((g - CORES * k) % groups, t))

    def flip(values, bits):
        return send(values, lambda g, t: (g, t ^ bits))

    out_rows = out_grad.reshape(-1, out_grad.shape[2])
    in_rows = layer_input.reshape(-1, layer_input.shape[2])
    gate_act = silu_gate.reshape(-1, hidden_width)
    up_value = up_proj.reshape(-1, hidden_width)
    rows = out_rows.shape[0]

    tops = range(per_chip, places, per_chip)
    middle = range(per_block, per_chip, per_block)
    near = range(1, per_block)
    pieces, crossing = {0: out_rows}, {0: in_rows}
    for m in tops:
        pieces[m] = flip(out_rows, m)
    for m in tops:
        crossing[m] = flip(in_rows, m)
    for n in middle:
        pieces[n] = flip(out_rows, n)
        for m in tops:
            pieces[m + n] = flip(pieces[m], n)
    for j in near:
        pieces[j] = flip(out_rows, j)
        for m in tops:
            pieces[m + j] = flip(pieces[m], j)
        for n in middle:
            pieces[n + j] = flip(pieces[n], j)
            for m in tops:
                pieces[m + n + j] = flip(pieces[m + n], j)

    spot, mine = place.astype(jnp.int32)[None], group.astype(jnp.int32)[None]
    far_w, far_gate, far_up, far_codes = (
        pltpu.with_memory_space_constraint(a, pltpu.HBM) for a in (w_down, gate_act, up_value, slope_codes)
    )
    w_here, hidden = first_half(spot, mine, far_w, far_gate, far_up)
    w_here, scaled_up = second_half(far_w, far_up, far_codes, w_here)

    def all_groups(values):
        found = [values, other_core(values)]
        for k in range(1, chips):
            received = from_chip(values, k)
            found += [received, other_core(received)]
        return found

    hidden_all = all_groups(hidden)

    def to_chip(k, m):
        return lambda t, g: jnp.bitwise_xor(t, m) // per_chip == (g // CORES + chips - k) % chips

    masks = [0] + list(tops)
    moves = []
    for k in range(chips):
        for i, m in enumerate(masks):
            moves.append((k, 0, i, 0, to_chip(k, m)))
            if k:
                moves.append((k, 1, len(masks) + i, 0, to_chip(k, m)))
    kept, *leaving = arrange(
        spot, mine, [crossing[m] for m in masks] + [pieces[m] for m in masks], rows, [1] + [2] * (chips - 1),
        moves,
    )

    def holds(t, g):
        return (t // per_block) % CORES == g % CORES

    def to_block(held):
        count = held.shape[0] // rows
        received = send(held, lambda g, t: (g, t ^ per_block) if (t // per_block) % CORES == g % CORES else None)
        moves = []
        for n in range(count):
            moves.append((0, n, 0, n, holds))
            moves.append((0, n, 1, n, lambda t, g: jnp.logical_not(holds(t, g))))
        (held,) = arrange(spot, mine, [held, received], rows, [count], moves)
        return [held] + [flip(held, j) for j in near]

    pair = [kept, other_core(kept)]
    (held,) = arrange(spot, mine, pair, rows, [2], [(0, c, c, 0, None) for c in range(CORES)])
    own_block = to_block(held)

    def to_neighbour(own, c):
        def target(g, t):
            holder = (t // per_block) % CORES == g % CORES
            return (g ^ c, t ^ per_block) if holder == own else None

        return target

    def spread(held, blocks, outputs, place_of):
        sources, moves = [], []
        for n, values in enumerate(held):
            for c in range(CORES):
                here = values if not c else other_core(values)
                there = send(values, to_neighbour(not c, c))
                for array, condition in ((here, holds), (there, lambda t, g: jnp.logical_not(holds(t, g)))):
                    for j in range(values.shape[0] // rows):
                        output, at = place_of(n * CORES + c, j)
                        moves.append((output, at, len(sources), j, condition))
                    sources.append(array)
        return arrange(spot, mine, sources, rows, [blocks] * outputs, moves)

    count = (chips - 1) * CORES
    in_crossed, out_crossed = [], []
    for k in range(1, chips):
        both = from_chip(leaving[k - 1], k)
        parts = arrange(spot, mine, [both], rows, [1, 1], [(0, 0, 0, 0, None), (1, 0, 0, 1, None)])
        in_crossed.append(parts[0])
        columns = [parts[1]] + [flip(parts[1], j) for j in near]
        if near:
            (columns,) = arrange(spot, mine, columns, rows, [per_block], [(0, j, j, 0, None) for j in range(per_block)])
        else:
            (columns,) = columns
        out_crossed.append(columns)
    (in_held,) = spread(in_crossed, count, 1, lambda n, j: (0, n))
    in_block = [in_held] + [flip(in_held, j) for j in near]
    out_block = spread(out_crossed, count, per_block, lambda n, j: (j, n))

    pieces = [pieces[m] for m in range(places)]
    bounds = [sum(EIGHTHS[:i]) * hidden_width // 8 for i in range(len(EIGHTHS) + 1)]
    grads = []
    for i, begin in enumerate(bounds[:-1]):
        chunk_width = bounds[i + 1] - begin
        found, *blocks = hidden_grads(
            pieces, w_here, spot, mine, scaled_up, gate_act, begin, chunk_width, min(512, chunk_width),
            0 if i else per_block,
        )
        grads.append(found)
        if not i:
            kept, given = blocks
    grads = [all_groups(values) for values in grads]
    given = other_core(given)
    far = range((chips - 1) * CORES)
    outputs = [[(kept, j), (given, j)] + [(out_block[j], n) for n in far] for j in range(per_block)]
    inputs = [[(own_block[j], c) for c in range(CORES)] + [(in_block[j], n) for n in far] for j in range(per_block)]
    carried, size = [], hidden_width // DOWN_PARTS
    for i in range(DOWN_PARTS):
        carried = [
            down_grad(hidden_all, outputs, rows, spot, carried, i * size, size, min(DOWN_BLOCK, size))
        ]
    (grad_down,) = carried

    carried = []
    for i, values in enumerate(grads):
        block = min(512, values[0].shape[2])
        carried = gate_up_grad(inputs, values, rows, spot, carried, bounds[i], hidden_width, block)
    return (grad_down, carried[0], carried[1])


def layer(groups, places, *args):
    return shards(groups, places, *args)


def solution(mesh):
    return jax.shard_map(
        functools.partial(layer, mesh.shape["dp"], mesh.shape["tensor"]),
        mesh=mesh,
        in_specs=(
            P(None, "dp", "tensor"),
            P(None, "dp", "tensor"),
            P("tensor", None),
            P(None, "dp", "tensor"),
            P(None, "dp", "tensor"),
            P(None, "dp", "tensor"),
        ),
        out_specs=(P("tensor", "dp"), P("dp", "tensor"), P("dp", "tensor")),
        check_vma=False,
    )
```

```python
import functools

import jax
import jax.numpy as jnp
from jax import lax
from jax.experimental import pallas as pl
from jax.experimental.pallas import tpu as pltpu
from jax.sharding import PartitionSpec as P


SLOPE_LEVELS = (-0.09, 0.06, 0.22, 0.41, 0.6, 0.79, 0.96, 1.08)
AXES = ("dp", "tensor")
CORES = 2
EIGHTHS = (4, 4)
VMEM_LIMIT = 20
LANES = 128
EARLY = 16
DOWN_PARTS = 2
DOWN_BLOCK = 512


IN_VMEM = pl.BlockSpec(memory_space=pltpu.VMEM)
IN_HBM = pl.BlockSpec(memory_space=pltpu.HBM)
PARAMS = pltpu.CompilerParams(vmem_limit_bytes=VMEM_LIMIT << 20)


def first_part(place, group, w_down, gate_act, up_value):
    rows, hidden_width = up_value.shape
    early = w_down.shape[0] // EARLY

    def body(place_ref, group_ref, w_ref, gate_ref, up_ref, w_out, hidden_ref, gate_buf, up_buf, done):
        copies = [
            pltpu.make_async_copy(gate_ref, gate_buf, done.at[0]),
            pltpu.make_async_copy(up_ref, up_buf, done.at[1]),
            pltpu.make_async_copy(w_ref.at[pl.ds(0, early)], w_out.at[pl.ds(0, early)], done.at[2]),
        ]
        for copy in copies:
            copy.start()
        for copy in copies[:2]:
            copy.wait()
        hidden_ref[...] = (gate_buf[...].astype(jnp.float32) * up_buf[...].astype(jnp.float32)).astype(jnp.bfloat16)
        copies[2].wait()

    return pl.pallas_call(
        body,
        grid_spec=pltpu.PrefetchScalarGridSpec(
            num_scalar_prefetch=2,
            grid=(1,),
            in_specs=[IN_HBM] * 3,
            out_specs=[IN_VMEM] * 2,
            scratch_shapes=[pltpu.VMEM((rows, hidden_width), jnp.bfloat16)] * 2 + [pltpu.SemaphoreType.DMA((3,))],
        ),
        out_shape=[
            jax.ShapeDtypeStruct(w_down.shape, jnp.bfloat16),
            jax.ShapeDtypeStruct((rows, hidden_width), jnp.bfloat16),
        ],
        compiler_params=PARAMS,
        cost_estimate=pl.CostEstimate(flops=rows * hidden_width, bytes_accessed=2 * w_down.size, transcendentals=0),
        name="first_part",
    )(place, group, w_down, gate_act, up_value)


def second_part(w_down, up_value, codes, w_here, end):
    micro, words, hidden_width = codes.shape
    rows = up_value.shape[0]
    per_word = rows // (micro * words)
    early = w_down.shape[0] // EARLY

    def body(w_ref, up_ref, code_ref, held_ref, w_out, scaled_ref, up_buf, code_buf, level_ref, done):
        copies = [
            pltpu.make_async_copy(code_ref, code_buf, done.at[0]),
            pltpu.make_async_copy(up_ref, up_buf, done.at[1]),
            pltpu.make_async_copy(w_ref.at[pl.ds(early, end - early)], w_out.at[pl.ds(early, end - early)], done.at[2]),
        ]
        for copy in copies:
            copy.start()
        for copy in copies[:2]:
            copy.wait()

        def columns(n, carry):
            here = pl.ds(pl.multiple_of(n * LANES, LANES), LANES)
            for m in range(micro):
                packed = code_buf[m, :, here]
                for k in range(per_word):
                    piece = jnp.bitwise_and(jnp.right_shift(packed, 3 * k), 7)
                    level = jnp.full(piece.shape, SLOPE_LEVELS[0], jnp.float32)
                    for symbol in range(1, 8):
                        level = jnp.where(piece == symbol, jnp.float32(SLOPE_LEVELS[symbol]), level)
                    level_ref[pl.ds(m * words * per_word + k, words, per_word), :] = level
            scaled_ref[:, here] = up_buf[:, here].astype(jnp.float32) * level_ref[...]
            return carry

        lax.fori_loop(0, hidden_width // LANES, columns, 0)
        copies[2].wait()

    return pl.pallas_call(
        body,
        in_specs=[IN_HBM] * 3 + [IN_VMEM],
        out_specs=[IN_VMEM] * 2,
        out_shape=[
            jax.ShapeDtypeStruct(w_down.shape, jnp.bfloat16),
            jax.ShapeDtypeStruct((rows, hidden_width), jnp.float32),
        ],
        scratch_shapes=[
            pltpu.VMEM((rows, hidden_width), jnp.bfloat16),
            pltpu.VMEM(codes.shape, jnp.int32),
            pltpu.VMEM((rows, LANES), jnp.float32),
            pltpu.SemaphoreType.DMA((3,)),
        ],
        input_output_aliases={3: 0},
        compiler_params=PARAMS,
        cost_estimate=pl.CostEstimate(flops=rows * hidden_width, bytes_accessed=2 * w_down.size, transcendentals=0),
        name="second_part",
    )(w_down, up_value, codes, w_here)


def arrange(place, group, inputs, rows, blocks, moves):
    width = inputs[0].shape[1]

    def body(place_ref, group_ref, *refs):
        sources, targets = refs[: len(inputs)], refs[len(inputs) :]
        for target, at, source, start, condition in moves:

            def copy(target=target, at=at, source=source, start=start):
                values = sources[source][start * rows : (start + 1) * rows, :]
                targets[target][at * rows : (at + 1) * rows, :] = values

            if condition is None:
                copy()
            else:
                pl.when(condition(place_ref[0], group_ref[0]))(copy)

    return pl.pallas_call(
        body,
        grid_spec=pltpu.PrefetchScalarGridSpec(
            num_scalar_prefetch=2,
            grid=(1,),
            in_specs=[IN_VMEM] * len(inputs),
            out_specs=[IN_VMEM] * len(blocks),
        ),
        out_shape=[jax.ShapeDtypeStruct((count * rows, width), jnp.bfloat16) for count in blocks],
        compiler_params=PARAMS,
        cost_estimate=pl.CostEstimate(flops=rows * width, bytes_accessed=4 * rows * width, transcendentals=0),
    )(place, group, *inputs)


def hidden_grads(pieces, w_down, place, group, scaled_up, gate_act, begin, chunk_width, block, per_block, far_w):
    rows, part = pieces[0].shape
    count = len(pieces)
    width = part * count
    steps, end = chunk_width // block, begin + chunk_width
    late = w_down.shape[0] - end
    out_shape = [jax.ShapeDtypeStruct((2, rows, chunk_width), jnp.bfloat16)]
    more, scratch = [], []
    if far_w is not None:
        out_shape += [jax.ShapeDtypeStruct((per_block * rows, part), jnp.bfloat16)] * CORES
        out_shape += [jax.ShapeDtypeStruct(w_down.shape, jnp.bfloat16)]
        more, scratch = [far_w], [pltpu.SemaphoreType.DMA]

    def body(place_ref, group_ref, *refs):
        piece_refs, (w_ref, up_ref, gate_ref), outs = refs[:count], refs[count : count + 3], refs[count + 3 + len(more) :]
        step = pl.program_id(0)
        if more:
            copy = pltpu.make_async_copy(
                refs[count + 3].at[pl.ds(end, late)], outs[1 + CORES].at[pl.ds(end, late)], outs[-1]
            )

            @pl.when(step == 0)
            def _():
                copy.start()

        here = pl.ds(pl.multiple_of(begin + step * block, block), block)
        there = pl.ds(pl.multiple_of(step * block, block), block)
        found = None
        for m in range(count):
            at = pl.multiple_of(jnp.bitwise_xor(place_ref[0], m) * part, part)
            product = lax.dot_general(
                w_ref[here, pl.ds(at, part)], piece_refs[m][...], (((1,), (1,)), ((), ())),
                preferred_element_type=jnp.float32,
            )
            found = product if found is None else found + product
        found = found.T
        outs[0][0, :, there] = (found * up_ref[:, here]).astype(jnp.bfloat16)
        outs[0][1, :, there] = (found * gate_ref[:, here].astype(jnp.float32)).astype(jnp.bfloat16)
        if more:

            @pl.when(step == 0)
            def _():
                for m in range(count):
                    owner = jnp.bitwise_xor(place_ref[0], m) // per_block
                    j = m % per_block
                    for c in range(CORES):

                        @pl.when(owner == jnp.bitwise_xor(group_ref[0], c))
                        def _():
                            outs[1 + c][j * rows : (j + 1) * rows, :] = piece_refs[m][...]

            @pl.when(step == steps - 1)
            def _():
                copy.wait()

    return pl.pallas_call(
        body,
        grid_spec=pltpu.PrefetchScalarGridSpec(
            num_scalar_prefetch=2,
            grid=(steps,),
            in_specs=[IN_VMEM] * (count + 3) + [IN_HBM] * len(more),
            out_specs=[IN_VMEM] * len(out_shape),
            scratch_shapes=scratch,
        ),
        out_shape=out_shape,
        input_output_aliases={2 + count: 1 + CORES} if more else {},
        compiler_params=PARAMS,
        cost_estimate=pl.CostEstimate(
            flops=2 * rows * width * chunk_width, bytes_accessed=2 * width * chunk_width, transcendentals=0
        ),
        name="hidden_grads",
    )(place, group, *pieces, w_down, scaled_up, gate_act, *more)


def flattened(groups):
    flat = [item for group in groups for item in group]
    return [a for a, n in flat], [n for a, n in flat]


def down_grad(hidden, outputs, rows, place, carried, begin, size, block):
    count, parts = len(hidden), len(outputs)
    hidden_width = hidden[0].shape[1]
    part = outputs[0][0][0].shape[1]
    width = parts * part
    tokens = rows * count
    flat, spots = flattened(outputs)

    def body(place_ref, *refs):
        lefts, rights, out_ref, right_ref = refs[:count], refs[count : count + len(flat)], refs[-2], refs[-1]

        @pl.when(pl.program_id(0) == 0)
        def _():
            for j in range(parts):
                at = pl.multiple_of(jnp.bitwise_xor(lax.rem(place_ref[0], parts), j) * part, part)
                for n in range(count):
                    values = rights[j * count + n][pl.ds(spots[j * count + n] * rows, rows), :]
                    right_ref[n * rows : (n + 1) * rows, pl.ds(at, part)] = values

        here = pl.ds(pl.multiple_of(begin + pl.program_id(0) * block, block), block)
        left = jnp.concatenate([r[:, here] for r in lefts], axis=0)
        out_ref[...] = lax.dot_general(
            left, right_ref[...], (((0,), (0,)), ((), ())), preferred_element_type=jnp.float32
        ).astype(jnp.bfloat16)

    return pl.pallas_call(
        body,
        grid_spec=pltpu.PrefetchScalarGridSpec(
            num_scalar_prefetch=1,
            grid=(size // block,),
            in_specs=[IN_VMEM] * (count + len(flat)) + [pl.BlockSpec(memory_space=pl.ANY)] * len(carried),
            out_specs=pl.BlockSpec((block, width), lambda i, s: (begin // block + i, 0)),
            scratch_shapes=[pltpu.VMEM((tokens, width), jnp.bfloat16)],
        ),
        out_shape=jax.ShapeDtypeStruct((hidden_width, width), jnp.bfloat16),
        cost_estimate=pl.CostEstimate(
            flops=2 * tokens * size * width, bytes_accessed=2 * width * size, transcendentals=0
        ),
        input_output_aliases={1 + count + len(flat): 0} if carried else {},
        compiler_params=PARAMS,
        name="down_grad",
    )(place, *hidden, *flat, *carried)


def gate_up_grad(inputs, grads, rows, place, left, carried, begin, hidden_width, block):
    count, parts = len(grads), len(inputs)
    part = inputs[0][0][0].shape[1]
    tokens = rows * count
    width = parts * part
    chunk_width = grads[0].shape[2]
    steps, first = chunk_width // block, begin // block
    extra = len(carried)
    fresh = left is None
    flat, spots = flattened(inputs)
    lefts = flat if fresh else [left]

    def body(place_ref, *refs):
        in_refs, grad_refs = refs[: len(lefts)], refs[len(lefts) : len(lefts) + count]
        outs = refs[len(lefts) + count + extra :]
        left_ref = outs[2] if fresh else in_refs[0]
        if fresh:

            @pl.when(pl.program_id(0) == 0)
            def _():
                for j in range(parts):
                    at = pl.multiple_of(jnp.bitwise_xor(lax.rem(place_ref[0], parts), j) * part, part)
                    spread = range(j * count, (j + 1) * count)
                    values = jnp.concatenate([in_refs[n][pl.ds(spots[n] * rows, rows), :] for n in spread], axis=0)
                    left_ref[pl.ds(at, part), :] = values.T

        here = pl.ds(pl.multiple_of(pl.program_id(0) * block, block), block)
        for k in range(2):
            right = jnp.concatenate([r[k, :, here] for r in grad_refs], axis=0)
            outs[k][...] = lax.dot_general(
                left_ref[...], right, (((1,), (0,)), ((), ())), preferred_element_type=jnp.float32
            ).astype(jnp.bfloat16)

    return pl.pallas_call(
        body,
        grid_spec=pltpu.PrefetchScalarGridSpec(
            num_scalar_prefetch=1,
            grid=(steps,),
            in_specs=[IN_VMEM] * (len(lefts) + count) + [pl.BlockSpec(memory_space=pl.ANY)] * extra,
            out_specs=[pl.BlockSpec((width, block), lambda i, s: (0, first + i))] * 2 + [IN_VMEM] * fresh,
        ),
        out_shape=[jax.ShapeDtypeStruct((width, hidden_width), jnp.bfloat16)] * 2
        + [jax.ShapeDtypeStruct((width, tokens), jnp.bfloat16)] * fresh,
        input_output_aliases={1 + len(lefts) + count + k: k for k in range(extra)},
        cost_estimate=pl.CostEstimate(
            flops=4 * tokens * chunk_width * width, bytes_accessed=4 * width * chunk_width, transcendentals=0
        ),
        compiler_params=PARAMS,
        name="gate_up_grad",
    )(place, *lefts, *grads, *carried)


def shards(groups, places, out_grad, layer_input, w_down, silu_gate, up_proj, slope_codes):
    chips = groups // CORES
    per_block = places // groups
    per_chip = per_block * CORES
    hidden_width = w_down.shape[0]
    group, place = lax.axis_index("dp"), lax.axis_index("tensor")
    everyone = [(g, t) for g in range(groups) for t in range(places)]

    def send(values, target):
        pairs = []
        for g, t in everyone:
            to = target(g, t)
            if to is not None:
                pairs.append((g * places + t, to[0] * places + to[1]))
        return lax.ppermute(values, AXES, pairs)

    def other_core(values):
        return send(values, lambda g, t: (g ^ 1, t))

    def from_chip(values, k):
        return send(values, lambda g, t: ((g - CORES * k) % groups, t))

    def flip(values, bits):
        return send(values, lambda g, t: (g, t ^ bits))

    out_rows = out_grad.reshape(-1, out_grad.shape[2])
    in_rows = layer_input.reshape(-1, layer_input.shape[2])
    gate_act = silu_gate.reshape(-1, hidden_width)
    up_value = up_proj.reshape(-1, hidden_width)
    rows = out_rows.shape[0]

    tops = range(per_chip, places, per_chip)
    middle = range(per_block, per_chip, per_block)
    near = range(1, per_block)
    pieces, crossing = {0: out_rows}, {0: in_rows}
    for m in tops:
        pieces[m] = flip(out_rows, m)
    for m in tops:
        crossing[m] = flip(in_rows, m)
    for n in middle:
        pieces[n] = flip(out_rows, n)
        for m in tops:
            pieces[m + n] = flip(pieces[m], n)
    for j in near:
        pieces[j] = flip(out_rows, j)
        for m in tops:
            pieces[m + j] = flip(pieces[m], j)
        for n in middle:
            pieces[n + j] = flip(pieces[n], j)
            for m in tops:
                pieces[m + n + j] = flip(pieces[m + n], j)

    spot, mine = place.astype(jnp.int32)[None], group.astype(jnp.int32)[None]
    bounds = [sum(EIGHTHS[:i]) * hidden_width // 8 for i in range(len(EIGHTHS) + 1)]
    far_w, far_gate, far_up, far_codes = (
        pltpu.with_memory_space_constraint(a, pltpu.HBM) for a in (w_down, gate_act, up_value, slope_codes)
    )
    w_here, hidden = first_part(spot, mine, far_w, far_gate, far_up)
    w_here, scaled_up = second_part(far_w, far_up, far_codes, w_here, bounds[1])

    def all_groups(values):
        found = [values, other_core(values)]
        for k in range(1, chips):
            received = from_chip(values, k)
            found += [received, other_core(received)]
        return found

    hidden_all = all_groups(hidden)

    def to_chip(k, m):
        return lambda t, g: jnp.bitwise_xor(t, m) // per_chip == (g // CORES + chips - k) % chips

    masks = [0] + list(tops)
    moves = []
    for k in range(chips):
        for i, m in enumerate(masks):
            moves.append((k, 0, i, 0, to_chip(k, m)))
            if k:
                moves.append((k, 1, len(masks) + i, 0, to_chip(k, m)))
    kept, *leaving = arrange(
        spot, mine, [crossing[m] for m in masks] + [pieces[m] for m in masks], rows, [1] + [2] * (chips - 1),
        moves,
    )

    def holds(t, g):
        return (t // per_block) % CORES == g % CORES

    def to_block(held):
        count = held.shape[0] // rows
        received = send(held, lambda g, t: (g, t ^ per_block) if (t // per_block) % CORES == g % CORES else None)
        moves = []
        for n in range(count):
            moves.append((0, n, 0, n, holds))
            moves.append((0, n, 1, n, lambda t, g: jnp.logical_not(holds(t, g))))
        (held,) = arrange(spot, mine, [held, received], rows, [count], moves)
        return [held] + [flip(held, j) for j in near]

    pair = [kept, other_core(kept)]
    (held,) = arrange(spot, mine, pair, rows, [2], [(0, c, c, 0, None) for c in range(CORES)])
    own_block = to_block(held)

    def to_neighbour(own, c):
        def target(g, t):
            holder = (t // per_block) % CORES == g % CORES
            return (g ^ c, t ^ per_block) if holder == own else None

        return target

    def spread(held, blocks, outputs, place_of):
        sources, moves = [], []
        for n, values in enumerate(held):
            for c in range(CORES):
                here = values if not c else other_core(values)
                there = send(values, to_neighbour(not c, c))
                for array, condition in ((here, holds), (there, lambda t, g: jnp.logical_not(holds(t, g)))):
                    for j in range(values.shape[0] // rows):
                        output, at = place_of(n * CORES + c, j)
                        moves.append((output, at, len(sources), j, condition))
                    sources.append(array)
        return arrange(spot, mine, sources, rows, [blocks] * outputs, moves)

    count = (chips - 1) * CORES
    in_crossed, out_crossed = [], []
    for k in range(1, chips):
        both = from_chip(leaving[k - 1], k)
        parts = arrange(spot, mine, [both], rows, [1, 1], [(0, 0, 0, 0, None), (1, 0, 0, 1, None)])
        in_crossed.append(parts[0])
        columns = [parts[1]] + [flip(parts[1], j) for j in near]
        if near:
            (columns,) = arrange(spot, mine, columns, rows, [per_block], [(0, j, j, 0, None) for j in range(per_block)])
        else:
            (columns,) = columns
        out_crossed.append(columns)
    (in_held,) = spread(in_crossed, count, 1, lambda n, j: (0, n))
    in_block = [in_held] + [flip(in_held, j) for j in near]
    out_block = spread(out_crossed, count, per_block, lambda n, j: (j, n))

    pieces = [pieces[m] for m in range(places)]
    grads = []
    for i, begin in enumerate(bounds[:-1]):
        chunk_width = bounds[i + 1] - begin
        found, *blocks = hidden_grads(
            pieces, w_here, spot, mine, scaled_up, gate_act, begin, chunk_width, min(512, chunk_width),
            per_block, None if i else far_w,
        )
        grads.append(found)
        if not i:
            kept, given, w_here = blocks
    grads = [all_groups(values) for values in grads]
    given = other_core(given)
    far = range((chips - 1) * CORES)
    outputs = [[(kept, j), (given, j)] + [(out_block[j], n) for n in far] for j in range(per_block)]
    inputs = [[(own_block[j], c) for c in range(CORES)] + [(in_block[j], n) for n in far] for j in range(per_block)]
    carried, size = [], hidden_width // DOWN_PARTS
    for i in range(DOWN_PARTS):
        carried = [
            down_grad(hidden_all, outputs, rows, spot, carried, i * size, size, min(DOWN_BLOCK, size))
        ]
    (grad_down,) = carried

    carried, left = [], None
    for i, values in enumerate(grads):
        block = min(512, values[0].shape[2])
        carried = gate_up_grad(inputs, values, rows, spot, left, carried, bounds[i], hidden_width, block)
        left = carried[2] if left is None else left
        carried = carried[:2]
    return (grad_down, carried[0], carried[1])


def layer(groups, places, *args):
    return shards(groups, places, *args)


def solution(mesh):
    return jax.shard_map(
        functools.partial(layer, mesh.shape["dp"], mesh.shape["tensor"]),
        mesh=mesh,
        in_specs=(
            P(None, "dp", "tensor"),
            P(None, "dp", "tensor"),
            P("tensor", None),
            P(None, "dp", "tensor"),
            P(None, "dp", "tensor"),
            P(None, "dp", "tensor"),
        ),
        out_specs=(P("tensor", "dp"), P("dp", "tensor"), P("dp", "tensor")),
        check_vma=False,
    )
```
